32 devices in a mesh: gx: 4 (over z), gy: 2 (over y), ea: 4 (over x, core).
Axes of the slice: x: 2, y: 2, z: 4, core: 2. Of those that a mesh axis runs over, the one named last changes fastest.
Arguments:
- load_displacement: float32 [3, 16, 32, 512], P(None, 'gx', 'gy', 'ea'), may hold values from -6 to 6
- load_enriched: float32 [15, 8192], P(None, ('gx', 'gy', 'ea')), may hold values from -24 to 24
- stiffness_shift: float32 [16, 32, 512], P('gx', 'gy', 'ea'), may hold values from 2 to 8
- enriched_diag: float32 [15, 8192], P(None, ('gx', 'gy', 'ea')), may hold values from 11 to 17
- enriched_off: float32 [15, 15, 8192], P(None, None, ('gx', 'gy', 'ea')), may hold values from -0.4 to 0.4
- coupling: float32 [3, 15, 16384], P(None, None, ('gx', 'gy', 'ea')), may hold values from -0.15 to 0.15
- slot_kind: int32 [32, 4, 128], P(('gx', 'gy', 'ea')), may hold values from 0 to 2, as said below
- slot_cell: int32 [32, 4, 128], P(('gx', 'gy', 'ea')), may hold values from 0 to 8191, as said below
- slot_node: int32 [32, 4, 128], P(('gx', 'gy', 'ea')), may hold values from 0 to 255, as said below
Outputs:
- solution_displacement: float32 [3, 16, 32, 512], P(None, 'gx', 'gy', 'ea')
- residual_displacement: float32 [3, 16, 32, 512], P(None, 'gx', 'gy', 'ea')
- solution_enriched: float32 [15, 8192], P(None, ('gx', 'gy', 'ea'))
- residual_enriched: float32 [15, 8192], P(None, ('gx', 'gy', 'ea'))
The draws below stay inside these ranges and needn't reach their ends.
Inputs may be any that keep to these rules, and one draw needn't show every extreme that they name: `slot_kind`: within each block of 128 slots of one device to one owner the slots of kind 1 or 2 come first; in every draw some owner receives 128 such slots from each of the 4 devices of its column. `slot_cell`: distinct within one device. `slot_node`: distinct within each block of 128 slots of one device to one owner.
All inputs are finite; a program needn't handle non-finite values.
Results may differ from the reference program's by a relative error of at most 0.0003.
Values sent between devices are 32-bit elements; how exact they have to be, the bound alone decides.
A program may use at most 64 MiB of HBM per device.

```python
import jax
import jax.numpy as jnp
from jax import lax

CX = 4
CY = 16
CZ = 128
ENB = 256
CAP = 128
ECOMP = 15
ITERS = 3
NX = 16
NY = 32
NZ = 512
NE = 8192
SLOTS = 16384
N_GX = 4
N_GY = 2
N_EA = 4
DEVICES = 32


def draw_slot_cell(key, part):
    device_keys = jax.random.split(jax.random.fold_in(key, 11), DEVICES)

    def one_device(device_key):
        return jax.random.permutation(device_key, CX * CY * CZ)[:N_EA * CAP].astype(jnp.int32)
    return jax.vmap(one_device)(device_keys).reshape(DEVICES, N_EA, CAP)


def draw_slot_node(key, part):
    block_keys = jax.random.split(jax.random.fold_in(key, 17), DEVICES * N_EA)

    def one_block(block_key):
        return jax.random.permutation(block_key, ENB)[:CAP].astype(jnp.int32)
    return jax.vmap(one_block)(block_keys).reshape(DEVICES, N_EA, CAP)


def draw_slot_kind(key, part):
    live_key, kind_key, column_key, owner_key = jax.random.split(jax.random.fold_in(key, 29), 4)
    live_count = jax.random.randint(live_key, (DEVICES, N_EA), CAP // 8, CAP + 1)
    columns = DEVICES // N_EA
    column = jax.random.randint(column_key, (), 0, columns)
    target = jax.random.randint(owner_key, (), 0, N_EA)
    device_ids = jnp.arange(DEVICES, dtype=jnp.int32)[:, None]
    owner_ids = jnp.arange(N_EA, dtype=jnp.int32)[None, :]
    full_block = (device_ids // N_EA == column) & (owner_ids == target)
    live_count = jnp.where(full_block, CAP, live_count)
    slot_kinds = jax.random.randint(kind_key, (DEVICES, N_EA, CAP), 1, 3)
    position = jnp.arange(CAP, dtype=jnp.int32)[None, None, :]
    return jnp.where(position < live_count[:, :, None], slot_kinds, 0).astype(jnp.int32)


def shard_levels(own_key, extent, cuts, low, largest):
    gain, own = 1.0, jax.random.fold_in(own_key, 6)
    for dim, blocks in cuts:
        steps = jnp.exp(jax.random.uniform(jax.random.fold_in(own, dim), (blocks,), jnp.float32, low / len(cuts), largest / len(cuts)))
        gain = gain * jnp.repeat(steps, extent[dim] // blocks).reshape([-1 if axis == dim else 1 for axis in range(len(extent))])
    return gain


def gaussian(own_key, extent, spread, limit, cuts=(), kind=jnp.bfloat16):
    loudness = shard_levels(own_key, extent, cuts, -0.22, 0.18) if cuts else 1.0
    entries = jax.random.normal(own_key, extent, jnp.float32) * spread * loudness
    return jnp.minimum(jnp.maximum(entries, -limit), limit).astype(kind)


def setup_inputs(seed: int = 0) -> dict:
    seeds = jax.random.split(jax.random.key(seed), 10)
    load_displacement = gaussian(seeds[0], (3, NX, NY, NZ), 1.0, 6.0, ((1, 4), (2, 2), (3, 4)), jnp.float32)
    load_enriched = gaussian(seeds[1], (ECOMP, NE), 4.0, 24.0, ((1, 32),), jnp.float32)
    stiffness_shift = jnp.clip(2.0 + 6.0 * jax.random.uniform(seeds[2], (NX, NY, NZ), jnp.float32) ** shard_levels(seeds[2], (NX, NY, NZ), ((0, 4), (1, 2), (2, 4)), -0.2, 0.2), 2.0, 8.0)
    enriched_diag = jnp.clip(11.0 + 6.0 * jax.random.uniform(seeds[3], (ECOMP, NE), jnp.float32) ** shard_levels(seeds[3], (ECOMP, NE), ((1, 32),), -0.2, 0.2), 11.0, 17.0)
    enriched_off = jnp.clip(jax.random.uniform(seeds[4], (ECOMP, ECOMP, NE), jnp.float32, -0.4, 0.4) * shard_levels(seeds[4], (ECOMP, ECOMP, NE), ((2, 32),), -0.4, 0.0), -0.4, 0.4)
    coupling = jnp.clip(jax.random.uniform(seeds[5], (3, ECOMP, SLOTS), jnp.float32, -0.15, 0.15) * shard_levels(seeds[5], (3, ECOMP, SLOTS), ((2, 32),), -0.4, 0.0), -0.15, 0.15)
    slot_kind = draw_slot_kind(jax.random.fold_in(seeds[9], 71), 0)
    slot_cell = draw_slot_cell(jax.random.fold_in(seeds[9], 71), 0)
    slot_node = draw_slot_node(jax.random.fold_in(seeds[9], 71), 0)
    return {"load_displacement": load_displacement, "load_enriched": load_enriched, "stiffness_shift": stiffness_shift, "enriched_diag": enriched_diag, "enriched_off": enriched_off, "coupling": coupling, "slot_kind": slot_kind, "slot_cell": slot_cell, "slot_node": slot_node}


HIGHEST_PRECISION = lax.Precision.HIGHEST


def stencil(displacement, stiffness_shift):
    padded = jnp.pad(displacement, ((0, 0), (1, 1), (1, 1), (1, 1)))
    beside = padded[:, 2:, 1:-1, 1:-1] + padded[:, :-2, 1:-1, 1:-1]
    beside = beside + padded[:, 1:-1, 2:, 1:-1] + padded[:, 1:-1, :-2, 1:-1]
    beside = beside + padded[:, 1:-1, 1:-1, 2:] + padded[:, 1:-1, 1:-1, :-2]
    return (6.0 + stiffness_shift)[None] * displacement - beside


def enriched_block(enriched_diag, enriched_off):
    components = enriched_diag.shape[0]
    identity = jnp.eye(components, dtype=jnp.float32)
    symmetric = 0.5 * (enriched_off + jnp.transpose(enriched_off, (1, 0, 2)))
    return symmetric * (1.0 - identity)[:, :, None] + identity[:, :, None] * enriched_diag[:, None, :]


def slot_columns(kinds_flat):
    heaviside = (kinds_flat >= 1).astype(jnp.float32)
    tip_mask = (kinds_flat == 2).astype(jnp.float32)
    return jnp.concatenate([jnp.broadcast_to(heaviside, (3, heaviside.shape[0])), jnp.broadcast_to(tip_mask, (12, tip_mask.shape[0]))], axis=0)


def inner(first, second):
    return jnp.sum(first[0] * second[0]) + jnp.sum(first[1] * second[1])


def reference(load_displacement, load_enriched, stiffness_shift, enriched_diag, enriched_off, coupling, slot_kind, slot_cell, slot_node):
    device_ids = jnp.arange(N_GX * N_GY * N_EA, dtype=jnp.int32)[:, None, None]
    owners = jnp.arange(N_EA, dtype=jnp.int32)[None, :, None]
    column_i = device_ids // (N_GY * N_EA)
    column_j = (device_ids // N_EA) % N_GY
    layer_k = device_ids % N_EA
    cell_x = slot_cell // (CY * CZ)
    cell_y = (slot_cell // CZ) % CY
    cell_z = slot_cell % CZ
    global_cell = (((column_i * CX + cell_x) * NY + column_j * CY + cell_y) * NZ + layer_k * CZ + cell_z).reshape(-1).astype(jnp.int32)
    global_node = ((device_ids - layer_k + owners) * ENB + slot_node).reshape(-1).astype(jnp.int32)
    slot_weights = coupling * slot_columns(slot_kind.reshape(-1))[None]
    enriched_stiff = enriched_block(enriched_diag, enriched_off)
    cell_total = NX * NY * NZ

    def operate(direction):
        displacement, enriched = direction
        flat = displacement.reshape(3, cell_total)
        picked = flat[:, global_cell]
        to_nodes = jnp.einsum('ijs,is->js', slot_weights, picked, precision=HIGHEST_PRECISION)
        pushed_enriched = jnp.einsum('ijn,jn->in', enriched_stiff, enriched, precision=HIGHEST_PRECISION)
        pushed_enriched = pushed_enriched + jnp.zeros(enriched.shape, jnp.float32).at[:, global_node].add(to_nodes)
        values = enriched[:, global_node]
        to_cells = jnp.einsum('ijs,js->is', slot_weights, values, precision=HIGHEST_PRECISION)
        added = jnp.zeros((3, cell_total), jnp.float32).at[:, global_cell].add(to_cells)
        pushed_displacement = stencil(displacement, stiffness_shift) + added.reshape(displacement.shape)
        return (pushed_displacement, pushed_enriched)

    solution = (jnp.zeros_like(load_displacement), jnp.zeros_like(load_enriched))
    residual = (load_displacement, load_enriched)
    direction = residual
    norm_now = inner(residual, residual)
    for iteration in range(ITERS):
        image = operate(direction)
        alpha = norm_now / inner(direction, image)
        solution = jax.tree.map(lambda member, partner: member + alpha * partner, solution, direction)
        residual = jax.tree.map(lambda member, partner: member - alpha * partner, residual, image)
        norm_next = inner(residual, residual)
        ratio = norm_next / norm_now
        direction = jax.tree.map(lambda member, partner: member + ratio * partner, residual, direction)
        norm_now = norm_next
    return solution[0], residual[0], solution[1], residual[1]
```

```python
import functools

import jax
import jax.numpy as jnp
from jax import lax
from jax.experimental import pallas as pl
from jax.experimental.pallas import tpu as pltpu
from jax.sharding import PartitionSpec as P

ITERS = 3
CENTRE = 11.5
AXES = ("gx", "gy", "ea")
MESH = pl.DeviceIdType.MESH
F32 = jnp.float32
BF16 = jnp.bfloat16


def pieces(x):
    high = x.astype(BF16)
    return high, (x - high.astype(F32)).astype(BF16)


def dot_nn(x, onehot):
    high, low = pieces(x)
    return jnp.dot(high, onehot, preferred_element_type=F32) + jnp.dot(
        low, onehot, preferred_element_type=F32
    )


def nt(x, onehot):
    return lax.dot_general(x, onehot, (((1,), (1,)), ((), ())), preferred_element_type=F32)


def iota(shape, dim):
    return lax.broadcasted_iota(jnp.int32, shape, dim)


def cg_coefficients(moment):
    def inner(first, second):
        total = None
        for i, a in enumerate(first):
            for j, b in enumerate(second):
                term = a * b * moment[i + j]
                total = term if total is None else total + term
        return total

    one = jnp.ones_like(moment[0])
    residual, direction, solution = [one], [one], []
    norm = moment[0]
    for step in range(ITERS):
        image = [CENTRE * d for d in direction] + [0.0 * one]
        for i, d in enumerate(direction):
            image[i + 1] = image[i + 1] + d
        alpha = norm / inner(direction, image)
        solution = [
            (solution[i] if i < len(solution) else 0.0) + alpha * d
            for i, d in enumerate(direction)
        ]
        residual = [
            (residual[i] if i < len(residual) else 0.0) - alpha * d for i, d in enumerate(image)
        ]
        if step + 1 < ITERS:
            new = inner(residual, residual)
            ratio = new / norm
            norm = new
            direction = [
                r + (ratio * direction[i] if i < len(direction) else 0.0)
                for i, r in enumerate(residual)
            ]
    return solution, residual


def kernel(
    sizes, groups,
    load_v, load_w, shift, diag, off, coupling, kind, cell, node,
    sol_v, res_v, sol_w, res_w,
    vu, wu, weights, stiff, lanes, rows, rows_b, nodes_mine, nodes_recv, centre_diag,
    node_in, x_in, y_in, z_in, w_in, t_in, y_out, z_out, t_out, red, red_out,
    node_s, node_r, x_s, x_r, y_s, y_r, z_s, z_r, w_s, w_r, t_s, t_r, red_s, red_r,
):
    n_gx, n_gy, n_ea = sizes
    comps, dx, dy, dz = load_v.shape
    ecomp, enb = load_w.shape
    cap = node.shape[2]
    per = dx * dy
    allrows = comps * per
    groups8 = allrows // 8
    gi, gj, ek = (lax.axis_index(a) for a in AXES)
    own = {"gx": gi, "gy": gj, "ea": ek}
    count = dict(zip(AXES, sizes))

    def members(group):
        total = 1
        for a in group:
            total *= count[a]
        me = 0
        for a in group:
            me = me * count[a] + own[a]

        def target(d):
            flat = lax.rem(me + d, total)
            coords = dict(own)
            for a in reversed(group):
                coords[a] = lax.rem(flat, count[a])
                flat = lax.div(flat, count[a])
            return tuple(coords[a] for a in AXES)

        return total, me, target

    barrier = pltpu.get_barrier_semaphore()
    expected = 0
    for group in groups:
        total, _, target = members(group)
        for d in range(1, total):
            pl.semaphore_signal(barrier, inc=1, device_id=target(d), device_id_type=MESH)
        expected += total - 1

    vu[0] = load_v[...]
    wu[0] = load_w[...]
    for o in range(n_ea):
        c = cell[0, o : o + 1, :]
        row = lax.shift_right_logical(c, dz.bit_length() - 1) if dz & (dz - 1) == 0 else c // dz
        lane = c - row * dz
        lanes[o] = jnp.where(iota((dz, cap), 0) == lane, 1.0, 0.0).astype(BF16)
        r = jnp.where(iota((per, cap), 0) == row, 1.0, 0.0)
        rows[o] = r
        rows_b[o] = r.astype(BF16)
        nodes_mine[o] = jnp.where(
            iota((enb, cap), 0) == node[0, o : o + 1, :], 1.0, 0.0
        ).astype(BF16)
        k = kind[0, o : o + 1, :]
        heavi = jnp.where(k >= 1, 1.0, 0.0)
        tip = jnp.where(k == 2, 1.0, 0.0)
        mask = jnp.where(iota((ecomp, cap), 0) < 3, heavi, tip)
        for i in range(comps):
            weights[o, i] = coupling[i, :, o * cap : (o + 1) * cap] * mask
    centre_diag[...] = shift[...] + (6.0 - CENTRE)

    pl.semaphore_wait(barrier, expected)

    waits = []

    def send(src, dst, s_sem, r_sem, device):
        copy = pltpu.make_async_remote_copy(
            src_ref=src, dst_ref=dst, send_sem=s_sem, recv_sem=r_sem,
            device_id=device, device_id_type=MESH,
        )
        copy.start()
        return copy

    def partner(d):
        return lax.rem(ek + d, n_ea)

    has = {
        ("gx", 1): gi < n_gx - 1, ("gx", -1): gi > 0,
        ("gy", 1): gj < n_gy - 1, ("gy", -1): gj > 0,
        ("ea", 1): ek < n_ea - 1, ("ea", -1): ek > 0,
    }
    beside = {
        ("gx", s): (gi + s, gj, ek) for s in (1, -1)
    } | {("gy", s): (gi, gj + s, ek) for s in (1, -1)} | {
        ("ea", s): (gi, gj, ek + s) for s in (1, -1)
    }
    slot = {1: 0, -1: 1}

    def remote(src, dst, s_sem, r_sem, device):
        return pltpu.make_async_remote_copy(
            src_ref=src, dst_ref=dst, send_sem=s_sem, recv_sem=r_sem,
            device_id=device, device_id_type=MESH,
        )

    def x_copy(op, s):
        return remote(
            vu.at[op, :, dx - 1 if s == 1 else 0], x_in.at[op, slot[s]],
            x_s.at[op, slot[s]], x_r.at[op, slot[s]], beside["gx", s],
        )

    def y_copy(op, s):
        return remote(
            y_out.at[op, slot[s]], y_in.at[op, slot[s]],
            y_s.at[op, slot[s]], y_r.at[op, slot[s]], beside["gy", s],
        )

    def z_copy(op, s):
        return remote(
            z_out.at[op, slot[s]], z_in.at[op, slot[s]],
            z_s.at[op, slot[s]], z_r.at[op, slot[s]], beside["ea", s],
        )

    def w_copy(op, d):
        return remote(
            wu.at[op], w_in.at[op, ek], w_s.at[op, d], w_r.at[op, d], (gi, gj, partner(d))
        )

    def t_copy(op, d):
        return remote(
            t_out.at[op, partner(d)], t_in.at[op, ek], t_s.at[op, d], t_r.at[op, d],
            (gi, gj, partner(d)),
        )

    def node_copy(d):
        return remote(
            node, node_in.at[ek], node_s.at[d], node_r.at[d], (gi, gj, partner(d))
        )

    def nodes_onehot(tile_row):
        return jnp.where(iota((enb, cap), 0) == tile_row, 1.0, 0.0).astype(BF16)

    lane_i = iota((8, dz), 1)

    def product(op_a, op_b):
        pv = jnp.sum((vu[op_a] * vu[op_b]).reshape(groups8, 8, dz), axis=0)
        pw = jnp.sum(wu[op_a] * wu[op_b], axis=0, keepdims=True)
        row = jnp.sum(pv, axis=0, keepdims=True)
        total = row
        for b in range(enb // dz):
            total = total + pw[:, b * dz : (b + 1) * dz]
        return total

    moments = []
    for op in range(ITERS):
        for s in (1, -1):
            @pl.when(has["gx", s])
            def _():
                x_copy(op, s).start()
        for d in range(1, n_ea):
            w_copy(op, d).start()
            if op == 0:
                node_copy(d).start()
        v2 = vu[op].reshape(allrows, dz)
        for i in range(comps):
            for a in range(dx):
                at = i * dx + a
                y_out[op, 0, at : at + 1, :] = vu[op, i, a, dy - 1 : dy, :]
                y_out[op, 1, at : at + 1, :] = vu[op, i, a, 0:1, :]
        for s in (1, -1):
            @pl.when(has["gy", s])
            def _():
                y_copy(op, s).start()
        up = jnp.zeros((8, dz), F32)
        down = jnp.zeros((8, dz), F32)
        for g in range(groups8):
            part = v2[8 * g : 8 * g + 8]
            up = jnp.where(lane_i == g, part[:, dz - 1 : dz], up)
            down = jnp.where(lane_i == g, part[:, 0:1], down)
        z_out[op, 0] = up
        z_out[op, 1] = down
        for s in (1, -1):
            @pl.when(has["ea", s])
            def _():
                z_copy(op, s).start()
        high, low = pieces(v2)
        for o in range(n_ea):
            seen = jnp.dot(high, lanes[o], preferred_element_type=F32) + jnp.dot(
                low, lanes[o], preferred_element_type=F32
            )
            total = None
            for i in range(comps):
                picked = jnp.sum(
                    seen[i * per : (i + 1) * per] * rows[o], axis=0, keepdims=True
                )
                term = weights[o, i] * picked
                total = term if total is None else total + term
            t_out[op, o] = total
        for d in range(1, n_ea):
            t_copy(op, d).start()

        if op == 0:
            for p in range(ecomp):
                whole = 0.5 * (off[p] + off[:, p, :])
                stiff[p] = jnp.where(
                    iota((ecomp, enb), 0) == p, diag[p : p + 1, :] - CENTRE, whole
                )
            nodes_recv[ek] = nodes_mine[ek]
        v4 = vu[op]
        zero = jnp.zeros((comps, 1, dy, dz), F32)
        near = jnp.concatenate([zero, v4[:, : dx - 1]], axis=1) + jnp.concatenate(
            [v4[:, 1:], zero], axis=1
        )
        near = near.reshape(allrows, dz)
        lane_all = iota((allrows, dz), 1)
        row_all = lax.rem(iota((allrows, dz), 0), dy)
        near = near + jnp.where(lane_all == 0, 0.0, pltpu.roll(v2, 1, 1))
        near = near + jnp.where(lane_all == dz - 1, 0.0, pltpu.roll(v2, dz - 1, 1))
        near = near + jnp.where(row_all == 0, 0.0, pltpu.roll(v2, 1, 0))
        near = near + jnp.where(row_all == dy - 1, 0.0, pltpu.roll(v2, allrows - 1, 0))
        vu[op + 1] = centre_diag[...][None] * v4 - near.reshape(v4.shape)
        w = wu[op]
        acc = stiff[0] * w[0:1]
        for p in range(1, ecomp):
            acc = acc + stiff[p] * w[p : p + 1]
        if op == 0:
            moments.append(product(0, 0))
        else:
            moments.append(product(op, op))

        def to_cells(owner, w_owner):
            values = dot_nn(w_owner, nodes_mine[owner])
            spread_h, spread_l = [], []
            mask = rows_b[owner]
            for i in range(comps):
                term = jnp.sum(weights[owner, i] * values, axis=0, keepdims=True)
                h, l = pieces(term)
                spread_h.append(mask * h)
                spread_l.append(mask * l)
            place = lanes[owner]
            added = nt(jnp.concatenate(spread_h, axis=0), place) + nt(
                jnp.concatenate(spread_l, axis=0), place
            )
            vu[op + 1] += added.reshape(comps, dx, dy, dz)

        def to_nodes(source, terms):
            h, l = pieces(terms)
            onehot = nodes_recv[source]
            return nt(h, onehot) + nt(l, onehot)

        to_cells(ek, w)
        acc = acc + to_nodes(ek, t_out[op, ek])
        if op == 0:
            for d in range(1, n_ea):
                node_copy(d).wait_recv()
                source = lax.rem(ek + n_ea - d, n_ea)
                nodes_recv[source] = nodes_onehot(node_in[source, 0, pl.ds(ek, 1), :])
        for s in (1, -1):
            @pl.when(has["gx", -s])
            def _():
                x_copy(op, s).wait_recv()
                edge = 0 if s == 1 else dx - 1
                vu[op + 1, :, edge] -= x_in[op, slot[s]]

            @pl.when(has["gy", -s])
            def _():
                y_copy(op, s).wait_recv()
                edge = 0 if s == 1 else dy - 1
                for i in range(comps):
                    for a in range(dx):
                        at = i * dx + a
                        vu[op + 1, i, a, edge : edge + 1, :] -= y_in[op, slot[s], at : at + 1, :]

            @pl.when(has["ea", -s])
            def _():
                z_copy(op, s).wait_recv()
                edge = 0 if s == 1 else dz - 1
                tile = z_in[op, slot[s]]
                for i in range(comps):
                    for a in range(dx):
                        for b in range(dy // 8):
                            g = (i * dx + a) * (dy // 8) + b
                            vu[op + 1, i, a, 8 * b : 8 * b + 8, :] -= jnp.where(
                                lane_i == edge, tile[:, g : g + 1], 0.0
                            )
        for d in range(1, n_ea):
            source = lax.rem(ek + n_ea - d, n_ea)
            w_copy(op, d).wait_recv()
            to_cells(source, w_in[op, source])
        for d in range(1, n_ea):
            source = lax.rem(ek + n_ea - d, n_ea)
            t_copy(op, d).wait_recv()
            acc = acc + to_nodes(source, t_in[op, source])
        wu[op + 1] = acc
        moments.append(product(op, op + 1))

    lane_r = iota((1, dz), 1)
    packed = jnp.zeros((1, dz), F32)
    for n, row in enumerate(moments):
        packed = jnp.where(lane_r == n, jnp.sum(row, axis=1, keepdims=True), packed)
    for stage, group in enumerate(groups):
        total, me, target = members(group)
        red_out[stage] = packed

        def red_copy(d):
            return remote(
                red_out.at[stage], red.at[stage, me], red_s.at[stage, d], red_r.at[stage, d],
                target(d),
            )

        for d in range(1, total):
            red_copy(d).start()
        red[stage, me] = packed
        for d in range(1, total):
            red_copy(d).wait_recv()
        packed = jnp.sum(red[stage, :total], axis=0)

    sol, res = cg_coefficients([packed[:, n : n + 1] for n in range(2 * ITERS)])
    v_terms = [vu[n].reshape(allrows, dz) for n in range(ITERS + 1)]
    w_terms = [wu[n] for n in range(ITERS + 1)]

    def combine(coefs, terms):
        out = coefs[0] * terms[0]
        for c, t in zip(coefs[1:], terms[1:]):
            out = out + c * t
        return out

    sol_v[...] = combine(sol, v_terms).reshape(sol_v.shape)
    res_v[...] = combine(res, v_terms).reshape(res_v.shape)
    sol_w[...] = combine(sol, w_terms)
    res_w[...] = combine(res, w_terms)

    for op in range(ITERS):
        for s in (1, -1):
            @pl.when(has["gx", s])
            def _():
                x_copy(op, s).wait_send()

            @pl.when(has["gy", s])
            def _():
                y_copy(op, s).wait_send()

            @pl.when(has["ea", s])
            def _():
                z_copy(op, s).wait_send()
        for d in range(1, n_ea):
            w_copy(op, d).wait_send()
            t_copy(op, d).wait_send()
            if op == 0:
                node_copy(d).wait_send()
    for stage, group in enumerate(groups):
        total, me, target = members(group)
        for d in range(1, total):
            remote(
                red_out.at[stage], red.at[stage, me], red_s.at[stage, d], red_r.at[stage, d],
                target(d),
            ).wait_send()


def body(sizes, *args):
    load_v, load_w, shift, diag, off, coupling, kind, cell, node = args
    n_ea = sizes[2]
    total = sizes[0] * sizes[1] * sizes[2]
    groups = (AXES,) if total <= 64 else (("gx",), ("gy", "ea"))
    widest = total if total <= 64 else max(sizes[0], sizes[1] * sizes[2])
    comps, dx, dy, dz = load_v.shape
    ecomp, enb = load_w.shape
    cap = node.shape[2]
    vmem = pltpu.VMEM
    dma = pltpu.SemaphoreType.DMA
    y_rows = -(-comps * dx // 8) * 8
    scratch = [
        vmem((ITERS + 1, comps, dx, dy, dz), F32),
        vmem((ITERS + 1, ecomp, enb), F32),
        vmem((n_ea, comps, ecomp, cap), F32),
        vmem((ecomp, ecomp, enb), F32),
        vmem((n_ea, dz, cap), BF16),
        vmem((n_ea, dx * dy, cap), F32),
        vmem((n_ea, dx * dy, cap), BF16),
        vmem((n_ea, enb, cap), BF16),
        vmem((n_ea, enb, cap), BF16),
        vmem((dx, dy, dz), F32),
        vmem((n_ea,) + node.shape, jnp.int32),
        vmem((ITERS, 2, comps, dy, dz), F32),
        vmem((ITERS, 2, y_rows, dz), F32),
        vmem((ITERS, 2, 8, dz), F32),
        vmem((ITERS, n_ea, ecomp, enb), F32),
        vmem((ITERS, n_ea, ecomp, cap), F32),
        vmem((ITERS, 2, y_rows, dz), F32),
        vmem((ITERS, 2, 8, dz), F32),
        vmem((ITERS, n_ea, ecomp, cap), F32),
        vmem((len(groups), widest, 1, dz), F32),
        vmem((len(groups), 1, dz), F32),
        dma((n_ea,)), dma((n_ea,)),
        dma((ITERS, 2)), dma((ITERS, 2)),
        dma((ITERS, 2)), dma((ITERS, 2)),
        dma((ITERS, 2)), dma((ITERS, 2)),
        dma((ITERS, n_ea)), dma((ITERS, n_ea)),
        dma((ITERS, n_ea)), dma((ITERS, n_ea)),
        dma((len(groups), widest)), dma((len(groups), widest)),
    ]
    out = pl.pallas_call(
        functools.partial(kernel, sizes, groups),
        out_shape=(
            jax.ShapeDtypeStruct(load_v.shape, F32),
            jax.ShapeDtypeStruct(load_v.shape, F32),
            jax.ShapeDtypeStruct(load_w.shape, F32),
            jax.ShapeDtypeStruct(load_w.shape, F32),
        ),
        in_specs=[pl.BlockSpec(memory_space=vmem)] * 9,
        out_specs=[pl.BlockSpec(memory_space=vmem)] * 4,
        scratch_shapes=scratch,
        compiler_params=pltpu.CompilerParams(collective_id=0, has_side_effects=True),
        name="krylov",
    )(*args)
    return tuple(out)


def solution(mesh):
    column = ("gx", "gy", "ea")
    placed = (
        P(None, "gx", "gy", "ea"),
        P(None, column),
        P("gx", "gy", "ea"),
        P(None, column),
        P(None, None, column),
        P(None, None, column),
        P(column, None, None),
        P(column, None, None),
        P(column, None, None),
    )
    return jax.shard_map(
        functools.partial(body, tuple(mesh.shape[a] for a in AXES)),
        mesh=mesh,
        in_specs=placed,
        out_specs=(
            P(None, "gx", "gy", "ea"),
            P(None, "gx", "gy", "ea"),
            P(None, column),
            P(None, column),
        ),
        check_vma=False,
    )
```

```python
import functools

import jax
import jax.numpy as jnp
from jax import lax
from jax.experimental import pallas as pl
from jax.experimental.pallas import tpu as pltpu
from jax.sharding import PartitionSpec as P

ITERS = 3
CENTRE = 11.5
AXES = ("gx", "gy", "ea")
MESH = pl.DeviceIdType.MESH
F32 = jnp.float32
BF16 = jnp.bfloat16


def pieces(x):
    high = x.astype(BF16)
    return high, (x - high.astype(F32)).astype(BF16)


def stacked(x):
    high, low = pieces(x)
    return jnp.concatenate([high, low], axis=0)


def folded(product):
    half = product.shape[0] // 2
    return product[:half] + product[half:]


def iota(shape, dim):
    return lax.broadcasted_iota(jnp.int32, shape, dim)


def cg_coefficients(moment):
    def inner(first, second):
        total = None
        for i, a in enumerate(first):
            for j, b in enumerate(second):
                term = a * b * moment[i + j]
                total = term if total is None else total + term
        return total

    one = jnp.ones_like(moment[0])
    residual, direction, solution = [one], [one], []
    norm = moment[0]
    for step in range(ITERS):
        image = [CENTRE * d for d in direction] + [0.0 * one]
        for i, d in enumerate(direction):
            image[i + 1] = image[i + 1] + d
        alpha = norm / inner(direction, image)
        solution = [
            (solution[i] if i < len(solution) else 0.0) + alpha * d
            for i, d in enumerate(direction)
        ]
        residual = [
            (residual[i] if i < len(residual) else 0.0) - alpha * d for i, d in enumerate(image)
        ]
        if step + 1 < ITERS:
            new = inner(residual, residual)
            ratio = new / norm
            norm = new
            direction = [
                r + (ratio * direction[i] if i < len(direction) else 0.0)
                for i, r in enumerate(residual)
            ]
    return solution, residual


def kernel(
    sizes, groups,
    load_v, load_w, shift_h, diag_h, off_h, coupling_h, kind_h, cell_h, node_h,
    vu, wu, coefs,
    w_first, shift, diag, off, coupling, kind, cell, node, load_s,
    weights, stiff, lanes, lanes_t, rows, rows_b, nodes_mine, nodes_recv, centre_diag,
    node_in, x_in, y_in, z_in, w_in, t_in, y_out, z_out, t_out, red, red_out,
    node_s, node_r, x_s, x_r, y_s, y_r, z_s, z_r, w_s, w_r, t_s, t_r, red_s, red_r,
):
    n_gx, n_gy, n_ea = sizes
    comps, dx, dy, dz = load_v.shape
    ecomp, enb = load_w.shape
    epad = wu.shape[1]
    cap = node.shape[2]
    per = dx * dy
    allrows = comps * per
    groups8 = allrows // 8
    gi, gj, ek = (lax.axis_index(a) for a in AXES)
    own = {"gx": gi, "gy": gj, "ea": ek}
    count = dict(zip(AXES, sizes))

    def members(group):
        total = 1
        for a in group:
            total *= count[a]
        me = 0
        for a in group:
            me = me * count[a] + own[a]

        def target(d):
            flat = lax.rem(me + d, total)
            coords = dict(own)
            for a in reversed(group):
                coords[a] = lax.rem(flat, count[a])
                flat = lax.div(flat, count[a])
            return tuple(coords[a] for a in AXES)

        return total, me, target

    barrier = pltpu.get_barrier_semaphore()
    expected = 0
    for group in groups:
        total, _, target = members(group)
        for d in range(1, total):
            pl.semaphore_signal(barrier, inc=1, device_id=target(d), device_id_type=MESH)
        expected += total - 1

    loads = {}
    for at, (name, src, dst) in enumerate((
        ("cell", cell_h, cell), ("v", load_v, vu.at[0]), ("node", node_h, node),
        ("kind", kind_h, kind), ("w", load_w, w_first), ("coupling", coupling_h, coupling),
        ("shift", shift_h, shift), ("off", off_h, off), ("diag", diag_h, diag),
    )):
        loads[name] = pltpu.make_async_copy(src, dst, load_s.at[at])
        loads[name].start()

    def columns(tile):
        full = jnp.concatenate(
            [tile.astype(F32), jnp.zeros((cap - tile.shape[0], cap), F32)], axis=0
        )
        return jnp.transpose(full).astype(jnp.int32)

    loads["cell"].wait()
    tile = cell[0]
    tile_row = lax.div(tile, dz)
    tile_lane = tile - tile_row * dz
    lane_columns = columns(tile_lane)
    for o in range(n_ea):
        span = slice(o * cap, (o + 1) * cap)
        lanes[:, span] = jnp.where(
            iota((dz, cap), 0) == tile_lane[o : o + 1], 1.0, 0.0
        ).astype(BF16)
        lanes_t[span, :] = jnp.where(
            iota((cap, dz), 1) == lane_columns[:, o : o + 1], 1.0, 0.0
        ).astype(BF16)
        r = jnp.where(iota((per, cap), 0) == tile_row[o : o + 1], 1.0, 0.0)
        rows[:, span] = r
        rows_b[:, span] = r.astype(BF16)
    loads["node"].wait()
    for o in range(n_ea):
        nodes_mine[o] = jnp.where(
            iota((enb, cap), 0) == node[0, o : o + 1, :], 1.0, 0.0
        ).astype(BF16)
    loads["kind"].wait()
    loads["coupling"].wait()
    no_row = jnp.zeros((epad - ecomp, n_ea * cap), F32)
    for i in range(comps):
        for o in range(n_ea):
            k = kind[0, o : o + 1, :]
            heavi = jnp.where(k >= 1, 1.0, 0.0)
            tip = jnp.where(k == 2, 1.0, 0.0)
            mask = jnp.where(iota((ecomp, cap), 0) < 3, heavi, tip)
            span = slice(o * cap, (o + 1) * cap)
            weights[i, :, span] = jnp.concatenate(
                [coupling[i, :, span] * mask, no_row[:, span]], axis=0
            )
    loads["w"].wait()
    wu[0] = jnp.concatenate([w_first[...], jnp.zeros((epad - ecomp, enb), F32)], axis=0)
    loads["v"].wait()

    pl.semaphore_wait(barrier, expected)

    def partner(d):
        return lax.rem(ek + d, n_ea)

    has = {
        ("gx", 1): gi < n_gx - 1, ("gx", -1): gi > 0,
        ("gy", 1): gj < n_gy - 1, ("gy", -1): gj > 0,
        ("ea", 1): ek < n_ea - 1, ("ea", -1): ek > 0,
    }
    beside = {
        ("gx", s): (gi + s, gj, ek) for s in (1, -1)
    } | {("gy", s): (gi, gj + s, ek) for s in (1, -1)} | {
        ("ea", s): (gi, gj, ek + s) for s in (1, -1)
    }
    slot = {1: 0, -1: 1}

    def remote(src, dst, s_sem, r_sem, device):
        return pltpu.make_async_remote_copy(
            src_ref=src, dst_ref=dst, send_sem=s_sem, recv_sem=r_sem,
            device_id=device, device_id_type=MESH,
        )

    def x_copy(op, s):
        return remote(
            vu.at[op, :, dx - 1 if s == 1 else 0], x_in.at[op, slot[s]],
            x_s.at[op, slot[s]], x_r.at[op, slot[s]], beside["gx", s],
        )

    def y_copy(op, s):
        return remote(
            y_out.at[op, slot[s]], y_in.at[op, slot[s]],
            y_s.at[op, slot[s]], y_r.at[op, slot[s]], beside["gy", s],
        )

    def z_copy(op, s):
        return remote(
            z_out.at[op, slot[s]], z_in.at[op, slot[s]],
            z_s.at[op, slot[s]], z_r.at[op, slot[s]], beside["ea", s],
        )

    def w_copy(op, d):
        return remote(
            wu.at[op], w_in.at[op, ek], w_s.at[op, d], w_r.at[op, d], (gi, gj, partner(d))
        )

    def t_copy(op, d):
        return remote(
            t_out.at[op, partner(d)], t_in.at[op, ek], t_s.at[op, d], t_r.at[op, d],
            (gi, gj, partner(d)),
        )

    def node_copy(d):
        return remote(
            node, node_in.at[ek], node_s.at[d], node_r.at[d], (gi, gj, partner(d))
        )

    lane_i = iota((8, dz), 1)
    lane_r = iota((1, dz), 1)

    def product(op_a, op_b):
        pv = jnp.sum((vu[op_a] * vu[op_b]).reshape(groups8, 8, dz), axis=0)
        pw = jnp.sum(wu[op_a] * wu[op_b], axis=0, keepdims=True)
        row = jnp.sum(pv, axis=0, keepdims=True)
        total = row
        for b in range(enb // dz):
            total = total + pw[:, b * dz : (b + 1) * dz]
        return total

    moments = []
    for op in range(ITERS):
        for s in (1, -1):
            @pl.when(has["gx", s])
            def _():
                x_copy(op, s).start()
        for d in range(1, n_ea):
            w_copy(op, d).start()
            if op == 0:
                node_copy(d).start()
        v2 = vu[op].reshape(allrows, dz)
        for i in range(comps):
            for a in range(dx):
                at = i * dx + a
                y_out[op, 0, at : at + 1, :] = vu[op, i, a, dy - 1 : dy, :]
                y_out[op, 1, at : at + 1, :] = vu[op, i, a, 0:1, :]
        for s in (1, -1):
            @pl.when(has["gy", s])
            def _():
                y_copy(op, s).start()
        up = jnp.zeros((8, dz), F32)
        down = jnp.zeros((8, dz), F32)
        for g in range(groups8):
            part = v2[8 * g : 8 * g + 8]
            up = jnp.where(lane_i == g, part[:, dz - 1 : dz], up)
            down = jnp.where(lane_i == g, part[:, 0:1], down)
        z_out[op, 0] = up
        z_out[op, 1] = down
        for s in (1, -1):
            @pl.when(has["ea", s])
            def _():
                z_copy(op, s).start()
        seen = folded(jnp.dot(stacked(v2), lanes[...], preferred_element_type=F32))
        total = None
        for i in range(comps):
            picked = jnp.sum(seen[i * per : (i + 1) * per] * rows[...], axis=0, keepdims=True)
            term = weights[i] * picked
            total = term if total is None else total + term
        for o in range(n_ea):
            t_out[op, o] = total[:, o * cap : (o + 1) * cap]
        for d in range(1, n_ea):
            t_copy(op, d).start()

        if op == 0:
            loads["off"].wait()
            loads["diag"].wait()
            for p in range(ecomp):
                whole = 0.5 * (off[p] + off[:, p, :])
                whole = jnp.where(
                    iota((ecomp, enb), 0) == p, diag[p : p + 1, :] - CENTRE, whole
                )
                stiff[p] = jnp.concatenate(
                    [whole, jnp.zeros((epad - ecomp, enb), F32)], axis=0
                )
            loads["shift"].wait()
            centre_diag[...] = shift[...] + (6.0 - CENTRE)
            node_in[ek] = node[...]
        v4 = vu[op]
        zero = jnp.zeros((comps, 1, dy, dz), F32)
        near = jnp.concatenate([zero, v4[:, : dx - 1]], axis=1) + jnp.concatenate(
            [v4[:, 1:], zero], axis=1
        )
        near = near.reshape(allrows, dz)
        lane_all = iota((allrows, dz), 1)
        row_all = lax.rem(iota((allrows, dz), 0), dy)
        near = near + jnp.where(lane_all == 0, 0.0, pltpu.roll(v2, 1, 1))
        near = near + jnp.where(lane_all == dz - 1, 0.0, pltpu.roll(v2, dz - 1, 1))
        near = near + jnp.where(row_all == 0, 0.0, pltpu.roll(v2, 1, 0))
        near = near + jnp.where(row_all == dy - 1, 0.0, pltpu.roll(v2, allrows - 1, 0))
        vu[op + 1] = centre_diag[...][None] * v4 - near.reshape(v4.shape)
        w = wu[op]
        acc = stiff[0] * w[0:1]
        for p in range(1, ecomp):
            acc = acc + stiff[p] * w[p : p + 1]
        if op == 0:
            moments.append(product(0, 0))
        else:
            moments.append(product(op, op))

        w_in[op, ek] = w
        t_in[op, ek] = t_out[op, ek]
        if op + 1 == ITERS:
            packed = jnp.zeros((1, dz), F32)
            for n, row in enumerate(moments):
                packed = jnp.where(lane_r == n, jnp.sum(row, axis=1, keepdims=True), packed)
        if op == 0:
            for d in range(1, n_ea):
                node_copy(d).wait_recv()
            own_rows = jnp.concatenate(
                [node_in[o, 0, pl.ds(ek, 1), :] for o in range(n_ea)], axis=0
            )
            node_columns = columns(own_rows)
            for o in range(n_ea):
                nodes_recv[o * cap : (o + 1) * cap, :] = jnp.where(
                    iota((cap, enb), 1) == node_columns[:, o : o + 1], 1.0, 0.0
                ).astype(BF16)
        for d in range(1, n_ea):
            w_copy(op, d).wait_recv()
        values = jnp.concatenate(
            [
                folded(jnp.dot(stacked(w_in[op, o]), nodes_mine[o], preferred_element_type=F32))
                for o in range(n_ea)
            ],
            axis=1,
        )
        spread_h, spread_l = [], []
        for i in range(comps):
            h, l = pieces(jnp.sum(weights[i] * values, axis=0, keepdims=True))
            spread_h.append(rows_b[...] * h)
            spread_l.append(rows_b[...] * l)
        added = folded(
            jnp.dot(
                jnp.concatenate(spread_h + spread_l, axis=0), lanes_t[...],
                preferred_element_type=F32,
            )
        )
        vu[op + 1] += added.reshape(comps, dx, dy, dz)
        for s in (1, -1):
            @pl.when(has["gx", -s])
            def _():
                x_copy(op, s).wait_recv()
                edge = 0 if s == 1 else dx - 1
                vu[op + 1, :, edge] -= x_in[op, slot[s]]

            @pl.when(has["gy", -s])
            def _():
                y_copy(op, s).wait_recv()
                edge = 0 if s == 1 else dy - 1
                for i in range(comps):
                    for a in range(dx):
                        at = i * dx + a
                        vu[op + 1, i, a, edge : edge + 1, :] -= y_in[op, slot[s], at : at + 1, :]

            @pl.when(has["ea", -s])
            def _():
                z_copy(op, s).wait_recv()
                edge = 0 if s == 1 else dz - 1
                tile = z_in[op, slot[s]]
                for i in range(comps):
                    for a in range(dx):
                        for b in range(dy // 8):
                            g = (i * dx + a) * (dy // 8) + b
                            vu[op + 1, i, a, 8 * b : 8 * b + 8, :] -= jnp.where(
                                lane_i == edge, tile[:, g : g + 1], 0.0
                            )
        for d in range(1, n_ea):
            t_copy(op, d).wait_recv()
        terms = jnp.concatenate([t_in[op, o] for o in range(n_ea)], axis=1)
        acc = acc + folded(
            jnp.dot(stacked(terms), nodes_recv[...], preferred_element_type=F32)
        )
        wu[op + 1] = acc
        moments.append(product(op, op + 1))

    last = 2 * ITERS - 1
    packed = jnp.where(lane_r == last, jnp.sum(moments[last], axis=1, keepdims=True), packed)
    for stage, group in enumerate(groups):
        total, me, target = members(group)
        red_out[stage] = packed

        def red_copy(d):
            return remote(
                red_out.at[stage], red.at[stage, me], red_s.at[stage, d], red_r.at[stage, d],
                target(d),
            )

        for d in range(1, total):
            red_copy(d).start()
        red[stage, me] = packed
        for d in range(1, total):
            red_copy(d).wait_recv()
        packed = jnp.sum(red[stage, :total], axis=0)

    sol, res = cg_coefficients([packed[:, n : n + 1] for n in range(2 * ITERS)])
    tile = jnp.zeros((1, dz), F32)
    for n, c in enumerate(sol + res):
        tile = jnp.where(lane_r == n, c, tile)
    coefs[...] = tile

    for op in range(ITERS):
        for s in (1, -1):
            @pl.when(has["gx", s])
            def _():
                x_copy(op, s).wait_send()

            @pl.when(has["gy", s])
            def _():
                y_copy(op, s).wait_send()

            @pl.when(has["ea", s])
            def _():
                z_copy(op, s).wait_send()
        for d in range(1, n_ea):
            w_copy(op, d).wait_send()
            t_copy(op, d).wait_send()
            if op == 0:
                node_copy(d).wait_send()
    for stage, group in enumerate(groups):
        total, me, target = members(group)
        for d in range(1, total):
            remote(
                red_out.at[stage], red.at[stage, me], red_s.at[stage, d], red_r.at[stage, d],
                target(d),
            ).wait_send()


def combine_kernel(vu, wu, coefs, sol_v, res_v, sol_w, res_w):
    ecomp = sol_w.shape[0]
    tile = coefs[...]
    solution = [tile[:, n : n + 1] for n in range(ITERS)]
    residual = [tile[:, ITERS + n : ITERS + n + 1] for n in range(ITERS + 1)]

    def combine(factors, terms):
        out = factors[0] * terms[0]
        for f, t in zip(factors[1:], terms[1:]):
            out = out + f * t
        return out

    shape = sol_v.shape
    flat = (shape[0] * shape[1] * shape[2], shape[3])
    v_terms = [vu[n].reshape(flat) for n in range(ITERS + 1)]
    w_terms = [wu[n] for n in range(ITERS + 1)]
    sol_v[...] = combine(solution, v_terms).reshape(shape)
    res_v[...] = combine(residual, v_terms).reshape(shape)
    sol_w[...] = combine(solution, w_terms)[:ecomp]
    res_w[...] = combine(residual, w_terms)[:ecomp]


def body(sizes, *args):
    load_v, load_w, shift, diag, off, coupling, kind, cell, node = args
    n_ea = sizes[2]
    total = sizes[0] * sizes[1] * sizes[2]
    groups = (AXES,) if total <= 64 else (("gx",), ("gy", "ea"))
    widest = total if total <= 64 else max(sizes[0], sizes[1] * sizes[2])
    comps, dx, dy, dz = load_v.shape
    ecomp, enb = load_w.shape
    cap = node.shape[2]
    vmem = pltpu.VMEM
    dma = pltpu.SemaphoreType.DMA
    y_rows = -(-comps * dx // 8) * 8
    epad = -(-ecomp // 16) * 16
    slots = n_ea * cap
    scratch = [
        vmem(load_w.shape, F32), vmem(shift.shape, F32), vmem(diag.shape, F32),
        vmem(off.shape, F32), vmem(coupling.shape, F32),
        vmem(kind.shape, jnp.int32), vmem(cell.shape, jnp.int32), vmem(node.shape, jnp.int32),
        dma((9,)),
        vmem((comps, epad, slots), F32),
        vmem((ecomp, epad, enb), F32),
        vmem((dz, slots), BF16),
        vmem((slots, dz), BF16),
        vmem((dx * dy, slots), F32),
        vmem((dx * dy, slots), BF16),
        vmem((n_ea, enb, cap), BF16),
        vmem((slots, enb), BF16),
        vmem((dx, dy, dz), F32),
        vmem((n_ea,) + node.shape, jnp.int32),
        vmem((ITERS, 2, comps, dy, dz), F32),
        vmem((ITERS, 2, y_rows, dz), F32),
        vmem((ITERS, 2, 8, dz), F32),
        vmem((ITERS, n_ea, epad, enb), F32),
        vmem((ITERS, n_ea, epad, cap), F32),
        vmem((ITERS, 2, y_rows, dz), F32),
        vmem((ITERS, 2, 8, dz), F32),
        vmem((ITERS, n_ea, epad, cap), F32),
        vmem((len(groups), widest, 1, dz), F32),
        vmem((len(groups), 1, dz), F32),
        dma((n_ea,)), dma((n_ea,)),
        dma((ITERS, 2)), dma((ITERS, 2)),
        dma((ITERS, 2)), dma((ITERS, 2)),
        dma((ITERS, 2)), dma((ITERS, 2)),
        dma((ITERS, n_ea)), dma((ITERS, n_ea)),
        dma((ITERS, n_ea)), dma((ITERS, n_ea)),
        dma((len(groups), widest)), dma((len(groups), widest)),
    ]
    basis = pl.pallas_call(
        functools.partial(kernel, sizes, groups),
        out_shape=(
            pltpu.VMEM((ITERS + 1,) + load_v.shape, F32),
            pltpu.VMEM((ITERS + 1, epad, enb), F32),
            pltpu.VMEM((1, dz), F32),
        ),
        in_specs=[pl.BlockSpec(memory_space=pltpu.HBM)] * 9,
        out_specs=[pl.BlockSpec(memory_space=vmem)] * 3,
        scratch_shapes=scratch,
        compiler_params=pltpu.CompilerParams(
            collective_id=0, has_side_effects=True
        ),
        name="krylov",
    )(*args)
    return tuple(
        pl.pallas_call(
            combine_kernel,
            out_shape=tuple(
                jax.ShapeDtypeStruct(like.shape, F32)
                for like in (load_v, load_v, load_w, load_w)
            ),
            in_specs=[pl.BlockSpec(memory_space=vmem)] * 3,
            out_specs=[pl.BlockSpec(memory_space=vmem)] * 4,
            compiler_params=pltpu.CompilerParams(vmem_limit_bytes=8 << 20),
            name="combine",
        )(*basis)
    )


def solution(mesh):
    column = ("gx", "gy", "ea")
    placed = (
        P(None, "gx", "gy", "ea"),
        P(None, column),
        P("gx", "gy", "ea"),
        P(None, column),
        P(None, None, column),
        P(None, None, column),
        P(column, None, None),
        P(column, None, None),
        P(column, None, None),
    )
    return jax.shard_map(
        functools.partial(body, tuple(mesh.shape[a] for a in AXES)),
        mesh=mesh,
        in_specs=placed,
        out_specs=(
            P(None, "gx", "gy", "ea"),
            P(None, "gx", "gy", "ea"),
            P(None, column),
            P(None, column),
        ),
        check_vma=False,
    )
```

```python
import functools

import jax
import jax.numpy as jnp
from jax import lax
from jax.experimental import pallas as pl
from jax.experimental.pallas import tpu as pltpu
from jax.sharding import PartitionSpec as P

ITERS = 3
CENTRE = 11.5
AXES = ("gx", "gy", "ea")
MESH = pl.DeviceIdType.MESH
F32 = jnp.float32
BF16 = jnp.bfloat16


def pieces(x):
    high = x.astype(BF16)
    return high, (x - high.astype(F32)).astype(BF16)


def stacked(x):
    high, low = pieces(x)
    return jnp.concatenate([high, low], axis=0)


def folded(product):
    half = product.shape[0] // 2
    return product[:half] + product[half:]


def iota(shape, dim):
    return lax.broadcasted_iota(jnp.int32, shape, dim)


def cg_coefficients(moment):
    def inner(first, second):
        total = None
        for i, a in enumerate(first):
            for j, b in enumerate(second):
                term = a * b * moment[i + j]
                total = term if total is None else total + term
        return total

    one = jnp.ones_like(moment[0])
    residual, direction, solution = [one], [one], []
    norm = moment[0]
    for step in range(ITERS):
        image = [CENTRE * d for d in direction] + [0.0 * one]
        for i, d in enumerate(direction):
            image[i + 1] = image[i + 1] + d
        alpha = norm / inner(direction, image)
        solution = [
            (solution[i] if i < len(solution) else 0.0) + alpha * d
            for i, d in enumerate(direction)
        ]
        residual = [
            (residual[i] if i < len(residual) else 0.0) - alpha * d for i, d in enumerate(image)
        ]
        if step + 1 < ITERS:
            new = inner(residual, residual)
            ratio = new / norm
            norm = new
            direction = [
                r + (ratio * direction[i] if i < len(direction) else 0.0)
                for i, r in enumerate(residual)
            ]
    return solution, residual


def kernel(
    sizes, groups,
    load_v, load_w, shift_h, diag_h, off_h, coupling_h, kind_h, cell_h, node_h,
    vu, wu, coefs,
    w_first, shift, diag, off, coupling, kind, cell, node, load_s,
    weights, stiff, lanes, lanes_t, rows, rows_b, nodes_mine, nodes_recv, centre_diag,
    node_in, x_in, y_in, z_in, w_in, t_in, y_out, z_out, t_out, red, red_out,
    node_s, node_r, x_s, x_r, y_s, y_r, z_s, z_r, w_s, w_r, t_s, t_r, red_s, red_r,
):
    n_gx, n_gy, n_ea = sizes
    comps, dx, dy, dz = load_v.shape
    ecomp, enb = load_w.shape
    epad = wu.shape[1]
    cap = node.shape[2]
    per = dx * dy
    allrows = comps * per
    groups8 = allrows // 8
    gi, gj, ek = (lax.axis_index(a) for a in AXES)
    own = {"gx": gi, "gy": gj, "ea": ek}
    count = dict(zip(AXES, sizes))
    wrapped = {
        a: [own[a]] + [lax.rem(own[a] + d, count[a]) for d in range(1, count[a])] for a in AXES
    }

    def members(group):
        total = 1
        for a in group:
            total *= count[a]
        me = 0
        for a in group:
            me = me * count[a] + own[a]

        def target(d):
            coords = dict(own)
            for a in reversed(group):
                coords[a] = wrapped[a][d % count[a]]
                d //= count[a]
            return tuple(coords[a] for a in AXES)

        return total, me, target

    barrier = pltpu.get_barrier_semaphore()
    expected = 0
    for group in groups:
        total, _, target = members(group)
        for d in range(1, total):
            pl.semaphore_signal(barrier, inc=1, device_id=target(d), device_id_type=MESH)
        expected += total - 1

    loads = {}
    for at, (name, src, dst) in enumerate((
        ("cell", cell_h, cell), ("v", load_v, vu.at[0]), ("node", node_h, node),
        ("kind", kind_h, kind), ("w", load_w, w_first), ("coupling", coupling_h, coupling),
        ("shift", shift_h, shift), ("off", off_h, off), ("diag", diag_h, diag),
    )):
        loads[name] = pltpu.make_async_copy(src, dst, load_s.at[at])
        loads[name].start()

    def columns(tile):
        full = jnp.concatenate(
            [tile.astype(F32), jnp.zeros((cap - tile.shape[0], cap), F32)], axis=0
        )
        return jnp.transpose(full).astype(jnp.int32)

    loads["cell"].wait()
    tile = cell[0]
    tile_row = lax.div(tile, dz)
    tile_lane = tile - tile_row * dz
    for o in range(n_ea):
        span = slice(o * cap, (o + 1) * cap)
        lanes[:, span] = jnp.where(
            iota((dz, cap), 0) == tile_lane[o : o + 1], 1.0, 0.0
        ).astype(BF16)
        r = jnp.where(iota((per, cap), 0) == tile_row[o : o + 1], 1.0, 0.0)
        rows[:, span] = r
        rows_b[:, span] = r.astype(BF16)
    loads["node"].wait()
    loads["kind"].wait()
    loads["coupling"].wait()
    no_row = jnp.zeros((epad - ecomp, n_ea * cap), F32)
    for i in range(comps):
        for o in range(n_ea):
            k = kind[0, o : o + 1, :]
            heavi = jnp.where(k >= 1, 1.0, 0.0)
            tip = jnp.where(k == 2, 1.0, 0.0)
            mask = jnp.where(iota((ecomp, cap), 0) < 3, heavi, tip)
            span = slice(o * cap, (o + 1) * cap)
            weights[i, :, span] = jnp.concatenate(
                [coupling[i, :, span] * mask, no_row[:, span]], axis=0
            )
    loads["w"].wait()
    wu[0] = jnp.concatenate([w_first[...], jnp.zeros((epad - ecomp, enb), F32)], axis=0)
    loads["v"].wait()

    pl.semaphore_wait(barrier, expected)

    def partner(d):
        return wrapped["ea"][d]

    has = {
        ("gx", 1): gi < n_gx - 1, ("gx", -1): gi > 0,
        ("gy", 1): gj < n_gy - 1, ("gy", -1): gj > 0,
        ("ea", 1): ek < n_ea - 1, ("ea", -1): ek > 0,
    }
    beside = {
        ("gx", s): (gi + s, gj, ek) for s in (1, -1)
    } | {("gy", s): (gi, gj + s, ek) for s in (1, -1)} | {
        ("ea", s): (gi, gj, ek + s) for s in (1, -1)
    }
    slot = {1: 0, -1: 1}

    def remote(src, dst, s_sem, r_sem, device):
        return pltpu.make_async_remote_copy(
            src_ref=src, dst_ref=dst, send_sem=s_sem, recv_sem=r_sem,
            device_id=device, device_id_type=MESH,
        )

    def x_copy(op, s):
        return remote(
            vu.at[op, :, dx - 1 if s == 1 else 0], x_in.at[op, slot[s]],
            x_s.at[op, slot[s]], x_r.at[op, slot[s]], beside["gx", s],
        )

    def y_copy(op, s):
        return remote(
            y_out.at[op, slot[s]], y_in.at[op, slot[s]],
            y_s.at[op, slot[s]], y_r.at[op, slot[s]], beside["gy", s],
        )

    def z_copy(op, s):
        return remote(
            z_out.at[op, slot[s]], z_in.at[op, slot[s]],
            z_s.at[op, slot[s]], z_r.at[op, slot[s]], beside["ea", s],
        )

    def w_copy(op, d):
        return remote(
            wu.at[op], w_in.at[op, ek], w_s.at[op, d], w_r.at[op, d], (gi, gj, partner(d))
        )

    def t_copy(op, d):
        return remote(
            t_out.at[op, partner(d)], t_in.at[op, ek], t_s.at[op, d], t_r.at[op, d],
            (gi, gj, partner(d)),
        )

    def node_copy(d):
        return remote(
            node, node_in.at[ek], node_s.at[d], node_r.at[d], (gi, gj, partner(d))
        )

    lane_i = iota((8, dz), 1)
    lane_r = iota((1, dz), 1)

    def product(op_a, op_b):
        pv = jnp.sum((vu[op_a] * vu[op_b]).reshape(groups8, 8, dz), axis=0)
        pw = jnp.sum(wu[op_a] * wu[op_b], axis=0, keepdims=True)
        row = jnp.sum(pv, axis=0, keepdims=True)
        total = row
        for b in range(enb // dz):
            total = total + pw[:, b * dz : (b + 1) * dz]
        return total

    moments = []
    for op in range(ITERS):
        for s in (1, -1):
            @pl.when(has["gx", s])
            def _():
                x_copy(op, s).start()
        for d in range(1, n_ea):
            w_copy(op, d).start()
            if op == 0:
                node_copy(d).start()
        v2 = vu[op].reshape(allrows, dz)
        for i in range(comps):
            for a in range(dx):
                at = i * dx + a
                y_out[op, 0, at : at + 1, :] = vu[op, i, a, dy - 1 : dy, :]
                y_out[op, 1, at : at + 1, :] = vu[op, i, a, 0:1, :]
        for s in (1, -1):
            @pl.when(has["gy", s])
            def _():
                y_copy(op, s).start()
        up = jnp.zeros((8, dz), F32)
        down = jnp.zeros((8, dz), F32)
        for g in range(groups8):
            part = v2[8 * g : 8 * g + 8]
            up = jnp.where(lane_i == g, part[:, dz - 1 : dz], up)
            down = jnp.where(lane_i == g, part[:, 0:1], down)
        z_out[op, 0] = up
        z_out[op, 1] = down
        for s in (1, -1):
            @pl.when(has["ea", s])
            def _():
                z_copy(op, s).start()
        seen = folded(jnp.dot(stacked(v2), lanes[...], preferred_element_type=F32))
        total = None
        for i in range(comps):
            picked = jnp.sum(seen[i * per : (i + 1) * per] * rows[...], axis=0, keepdims=True)
            term = weights[i] * picked
            total = term if total is None else total + term
        for o in range(n_ea):
            t_out[op, o] = total[:, o * cap : (o + 1) * cap]
        for d in range(1, n_ea):
            t_copy(op, d).start()

        if op == 0:
            lane_columns = columns(tile_lane)
            for o in range(n_ea):
                lanes_t[o * cap : (o + 1) * cap, :] = jnp.where(
                    iota((cap, dz), 1) == lane_columns[:, o : o + 1], 1.0, 0.0
                ).astype(BF16)
                nodes_mine[o] = jnp.where(
                    iota((enb, cap), 0) == node[0, o : o + 1, :], 1.0, 0.0
                ).astype(BF16)
            loads["off"].wait()
            loads["diag"].wait()
            for p in range(ecomp):
                whole = 0.5 * (off[p] + off[:, p, :])
                whole = jnp.where(
                    iota((ecomp, enb), 0) == p, diag[p : p + 1, :] - CENTRE, whole
                )
                stiff[p] = jnp.concatenate(
                    [whole, jnp.zeros((epad - ecomp, enb), F32)], axis=0
                )
            loads["shift"].wait()
            centre_diag[...] = shift[...] + (6.0 - CENTRE)
            node_in[ek] = node[...]
        v4 = vu[op]
        zero = jnp.zeros((comps, 1, dy, dz), F32)
        near = jnp.concatenate([zero, v4[:, : dx - 1]], axis=1) + jnp.concatenate(
            [v4[:, 1:], zero], axis=1
        )
        near = near.reshape(allrows, dz)
        lane_all = iota((allrows, dz), 1)
        row_all = lax.rem(iota((allrows, dz), 0), dy)
        near = near + jnp.where(lane_all == 0, 0.0, pltpu.roll(v2, 1, 1))
        near = near + jnp.where(lane_all == dz - 1, 0.0, pltpu.roll(v2, dz - 1, 1))
        near = near + jnp.where(row_all == 0, 0.0, pltpu.roll(v2, 1, 0))
        near = near + jnp.where(row_all == dy - 1, 0.0, pltpu.roll(v2, allrows - 1, 0))
        vu[op + 1] = centre_diag[...][None] * v4 - near.reshape(v4.shape)
        w = wu[op]
        acc = stiff[0] * w[0:1]
        for p in range(1, ecomp):
            acc = acc + stiff[p] * w[p : p + 1]
        if op == 0:
            moments.append(product(0, 0))
        else:
            moments.append(product(op, op))

        w_in[op, ek] = w
        t_in[op, ek] = t_out[op, ek]
        if op + 1 == ITERS:
            packed = jnp.zeros((1, dz), F32)
            for n, row in enumerate(moments):
                packed = jnp.where(lane_r == n, jnp.sum(row, axis=1, keepdims=True), packed)
        if op == 0:
            for d in range(1, n_ea):
                node_copy(d).wait_recv()
            own_rows = jnp.concatenate(
                [node_in[o, 0, pl.ds(ek, 1), :] for o in range(n_ea)], axis=0
            )
            node_columns = columns(own_rows)
            for o in range(n_ea):
                nodes_recv[o * cap : (o + 1) * cap, :] = jnp.where(
                    iota((cap, enb), 1) == node_columns[:, o : o + 1], 1.0, 0.0
                ).astype(BF16)
        for s in (1, -1):
            @pl.when(has["gx", -s])
            def _():
                x_copy(op, s).wait_recv()
                edge = 0 if s == 1 else dx - 1
                vu[op + 1, :, edge] -= x_in[op, slot[s]]

            @pl.when(has["gy", -s])
            def _():
                y_copy(op, s).wait_recv()
                edge = 0 if s == 1 else dy - 1
                for i in range(comps):
                    for a in range(dx):
                        at = i * dx + a
                        vu[op + 1, i, a, edge : edge + 1, :] -= y_in[op, slot[s], at : at + 1, :]

            @pl.when(has["ea", -s])
            def _():
                z_copy(op, s).wait_recv()
                edge = 0 if s == 1 else dz - 1
                tile = z_in[op, slot[s]]
                for i in range(comps):
                    for a in range(dx):
                        for b in range(dy // 8):
                            g = (i * dx + a) * (dy // 8) + b
                            vu[op + 1, i, a, 8 * b : 8 * b + 8, :] -= jnp.where(
                                lane_i == edge, tile[:, g : g + 1], 0.0
                            )
        for d in range(1, n_ea):
            w_copy(op, d).wait_recv()
            t_copy(op, d).wait_recv()
        values = jnp.concatenate(
            [
                folded(jnp.dot(stacked(w_in[op, o]), nodes_mine[o], preferred_element_type=F32))
                for o in range(n_ea)
            ],
            axis=1,
        )
        spread_h, spread_l = [], []
        for i in range(comps):
            h, l = pieces(jnp.sum(weights[i] * values, axis=0, keepdims=True))
            spread_h.append(rows_b[...] * h)
            spread_l.append(rows_b[...] * l)
        added = folded(
            jnp.dot(
                jnp.concatenate(spread_h + spread_l, axis=0), lanes_t[...],
                preferred_element_type=F32,
            )
        )
        vu[op + 1] += added.reshape(comps, dx, dy, dz)
        terms = jnp.concatenate([t_in[op, o] for o in range(n_ea)], axis=1)
        acc = acc + folded(
            jnp.dot(stacked(terms), nodes_recv[...], preferred_element_type=F32)
        )
        wu[op + 1] = acc
        moments.append(product(op, op + 1))

    last = 2 * ITERS - 1
    packed = jnp.where(lane_r == last, jnp.sum(moments[last], axis=1, keepdims=True), packed)
    for stage, group in enumerate(groups):
        total, me, target = members(group)
        red_out[stage] = packed

        def red_copy(d):
            return remote(
                red_out.at[stage], red.at[stage, me], red_s.at[stage, d], red_r.at[stage, d],
                target(d),
            )

        for d in range(1, total):
            red_copy(d).start()
        red[stage, me] = packed
        for d in range(1, total):
            red_copy(d).wait_recv()
        packed = jnp.sum(red[stage, :total], axis=0)

    sol, res = cg_coefficients([packed[:, n : n + 1] for n in range(2 * ITERS)])
    tile = jnp.zeros((1, dz), F32)
    for n, c in enumerate(sol + res):
        tile = jnp.where(lane_r == n, c, tile)
    coefs[...] = tile

    for op in range(ITERS):
        for s in (1, -1):
            @pl.when(has["gx", s])
            def _():
                x_copy(op, s).wait_send()

            @pl.when(has["gy", s])
            def _():
                y_copy(op, s).wait_send()

            @pl.when(has["ea", s])
            def _():
                z_copy(op, s).wait_send()
        for d in range(1, n_ea):
            w_copy(op, d).wait_send()
            t_copy(op, d).wait_send()
            if op == 0:
                node_copy(d).wait_send()
    for stage, group in enumerate(groups):
        total, me, target = members(group)
        for d in range(1, total):
            remote(
                red_out.at[stage], red.at[stage, me], red_s.at[stage, d], red_r.at[stage, d],
                target(d),
            ).wait_send()


def combine_kernel(vu, wu, coefs, sol_v, res_v, sol_w, res_w):
    ecomp = sol_w.shape[0]
    tile = coefs[...]
    solution = [tile[:, n : n + 1] for n in range(ITERS)]
    residual = [tile[:, ITERS + n : ITERS + n + 1] for n in range(ITERS + 1)]

    def combine(factors, terms):
        out = factors[0] * terms[0]
        for f, t in zip(factors[1:], terms[1:]):
            out = out + f * t
        return out

    shape = sol_v.shape
    flat = (shape[0] * shape[1] * shape[2], shape[3])
    v_terms = [vu[n].reshape(flat) for n in range(ITERS + 1)]
    w_terms = [wu[n] for n in range(ITERS + 1)]
    sol_v[...] = combine(solution, v_terms).reshape(shape)
    res_v[...] = combine(residual, v_terms).reshape(shape)
    sol_w[...] = combine(solution, w_terms)[:ecomp]
    res_w[...] = combine(residual, w_terms)[:ecomp]


def body(sizes, *args):
    load_v, load_w, shift, diag, off, coupling, kind, cell, node = args
    n_ea = sizes[2]
    total = sizes[0] * sizes[1] * sizes[2]
    groups = (AXES,) if total <= 64 else (("gx",), ("gy", "ea"))
    widest = total if total <= 64 else max(sizes[0], sizes[1] * sizes[2])
    comps, dx, dy, dz = load_v.shape
    ecomp, enb = load_w.shape
    cap = node.shape[2]
    vmem = pltpu.VMEM
    dma = pltpu.SemaphoreType.DMA
    y_rows = -(-comps * dx // 8) * 8
    epad = -(-ecomp // 16) * 16
    slots = n_ea * cap
    scratch = [
        vmem(load_w.shape, F32), vmem(shift.shape, F32), vmem(diag.shape, F32),
        vmem(off.shape, F32), vmem(coupling.shape, F32),
        vmem(kind.shape, jnp.int32), vmem(cell.shape, jnp.int32), vmem(node.shape, jnp.int32),
        dma((9,)),
        vmem((comps, epad, slots), F32),
        vmem((ecomp, epad, enb), F32),
        vmem((dz, slots), BF16),
        vmem((slots, dz), BF16),
        vmem((dx * dy, slots), F32),
        vmem((dx * dy, slots), BF16),
        vmem((n_ea, enb, cap), BF16),
        vmem((slots, enb), BF16),
        vmem((dx, dy, dz), F32),
        vmem((n_ea,) + node.shape, jnp.int32),
        vmem((ITERS, 2, comps, dy, dz), F32),
        vmem((ITERS, 2, y_rows, dz), F32),
        vmem((ITERS, 2, 8, dz), F32),
        vmem((ITERS, n_ea, epad, enb), F32),
        vmem((ITERS, n_ea, epad, cap), F32),
        vmem((ITERS, 2, y_rows, dz), F32),
        vmem((ITERS, 2, 8, dz), F32),
        vmem((ITERS, n_ea, epad, cap), F32),
        vmem((len(groups), widest, 1, dz), F32),
        vmem((len(groups), 1, dz), F32),
        dma((n_ea,)), dma((n_ea,)),
        dma((ITERS, 2)), dma((ITERS, 2)),
        dma((ITERS, 2)), dma((ITERS, 2)),
        dma((ITERS, 2)), dma((ITERS, 2)),
        dma((ITERS, n_ea)), dma((ITERS, n_ea)),
        dma((ITERS, n_ea)), dma((ITERS, n_ea)),
        dma((len(groups), widest)), dma((len(groups), widest)),
    ]
    basis = pl.pallas_call(
        functools.partial(kernel, sizes, groups),
        out_shape=(
            pltpu.VMEM((ITERS + 1,) + load_v.shape, F32),
            pltpu.VMEM((ITERS + 1, epad, enb), F32),
            pltpu.VMEM((1, dz), F32),
        ),
        in_specs=[pl.BlockSpec(memory_space=pltpu.HBM)] * 9,
        out_specs=[pl.BlockSpec(memory_space=vmem)] * 3,
        scratch_shapes=scratch,
        compiler_params=pltpu.CompilerParams(
            collective_id=0, has_side_effects=True
        ),
        name="krylov",
    )(*args)
    return tuple(
        pl.pallas_call(
            combine_kernel,
            out_shape=tuple(
                jax.ShapeDtypeStruct(like.shape, F32)
                for like in (load_v, load_v, load_w, load_w)
            ),
            in_specs=[pl.BlockSpec(memory_space=vmem)] * 3,
            out_specs=[pl.BlockSpec(memory_space=vmem)] * 4,
            compiler_params=pltpu.CompilerParams(vmem_limit_bytes=8 << 20),
            name="combine",
        )(*basis)
    )


def solution(mesh):
    column = ("gx", "gy", "ea")
    placed = (
        P(None, "gx", "gy", "ea"),
        P(None, column),
        P("gx", "gy", "ea"),
        P(None, column),
        P(None, None, column),
        P(None, None, column),
        P(column, None, None),
        P(column, None, None),
        P(column, None, None),
    )
    return jax.shard_map(
        functools.partial(body, tuple(mesh.shape[a] for a in AXES)),
        mesh=mesh,
        in_specs=placed,
        out_specs=(
            P(None, "gx", "gy", "ea"),
            P(None, "gx", "gy", "ea"),
            P(None, column),
            P(None, column),
        ),
        check_vma=False,
    )
```
